32 devices in a mesh: cell: 8 (over z, y), inst: 4 (over x, core).
Axes of the slice: x: 2, y: 2, z: 4, core: 2. Of those that a mesh axis runs over, the one named last changes fastest.
Arguments:
- fine_residual: float32 [8, 6, 65536], P('inst', None, 'cell'), may hold values from -6 to 6
- fine_map: int32 [65536], P('cell'), may hold values from 0 to 15
- routes: int32 [8, 64], P('cell'), may hold values from 0 to 7, as said below
- receive_lists: int32 [8, 192], P('cell'), may hold values from 0 to 1023
- neighbours: int32 [6, 8192], P(None, 'cell'), may hold values from 0 to 1215, as said below
- face_weights: float32 [6, 8192], P(None, 'cell'), may hold values from 0.3 to 3
- spectral_coef: float32 [8192], P('cell'), may hold values from 0.2 to 1
- diag_extra: float32 [6, 8192], P(None, 'cell'), may hold values from 0.5 to 2
Outputs:
- fine_correction: float32 [8, 6, 65536], P('inst', None, 'cell')
- coarse_correction: float32 [8, 6, 8192], P('inst', None, 'cell')
The draws below stay inside these ranges and needn't reach their ends.
Inputs may be any that keep to these rules, and one draw needn't show every extreme that they name: `routes`: in row p, the value p appears 64 - 2 * 4 times, and (p - 1) mod 8 and (p + 1) mod 8 appear 4 times each. `receive_lists`: row o, entries t * 32 to t * 32 + 31, list cells that partition o receives as halo from partition (o + d) mod 8, with d = t - 3 for t < 3 and d = t - 2 otherwise. `neighbours`: A value below 1024 is a cell of the own partition; a value x of 1024 or more is halo slot x - 1024.
All inputs are finite; a program needn't handle non-finite values.
Results may differ from the reference program's by a relative error of at most 0.0001.
Values sent between devices are 32-bit elements; how exact they have to be, the bound alone decides.
A program may use at most 64 MiB of HBM per device.

```python
import math
import jax
import jax.numpy as jnp
from jax import lax

VARS = 6
INST = 8
HB_INST = 7
NB = 6
AGG = 8
BLK = 128
RAD = 3
FB = 64
ITERS = 6
CBLK = 16
FINE = 65536
CC = 1024
COARSE = 8192
HS = 32
N_CELL = 8


def draw_routes(key, part):
    handed = FB // 16
    row_keys = jax.random.split(jax.random.fold_in(key, 17), N_CELL)

    def one_row(partition, row_key):
        slots = jnp.arange(FB, dtype=jnp.int32)
        below = jnp.mod(partition + N_CELL - 1, N_CELL)
        above = jnp.mod(partition + 1, N_CELL)
        owner_ids = jnp.where(slots < handed, below, jnp.where(slots < 2 * handed, above, partition))
        return jax.random.permutation(row_key, owner_ids)
    return jax.vmap(one_row)(jnp.arange(N_CELL, dtype=jnp.int32), row_keys).astype(jnp.int32)


def draw_neighbours(key, part):
    base = jax.random.fold_in(key, 29)
    local_key, halo_key, pick_key = jax.random.split(base, 3)
    local_ids = jax.random.randint(local_key, (NB, COARSE), 0, CC)
    halo_ids = CC + jax.random.randint(halo_key, (NB, COARSE), 0, 2 * RAD * HS)
    picked = jax.random.randint(pick_key, (NB, COARSE), 0, 5) < 4
    return jnp.where(picked, local_ids, halo_ids).astype(jnp.int32)


def touch_ends(values, rng, least, largest):
    shape = values.shape
    spot = [jax.random.randint(jax.random.fold_in(rng, axis), (), 0, shape[axis]) for axis in range(len(shape))]
    values = values.at[tuple(spot)].set(least)
    longest = shape.index(max(shape))
    spot[longest] = (spot[longest] + 1) % shape[longest]
    return values.at[tuple(spot)].set(largest)


def shard_levels(own_key, extent, cuts, low, top_value):
    def one(dim, parts):
        steps = jax.random.uniform(jax.random.fold_in(jax.random.fold_in(own_key, 6), dim), (parts,), jnp.float32, low / len(cuts), top_value / len(cuts))
        return jnp.repeat(jnp.exp(steps), extent[dim] // parts).reshape((-1,) + (1,) * (len(extent) - dim - 1))

    loudness = one(*cuts[0])
    for cut in cuts[1:]:
        loudness = loudness * one(*cut)
    return loudness


def scatter_about(rng, shape, spread, reach, pieces=(), held_as=jnp.bfloat16):
    drawn = spread * jax.random.normal(rng, shape, jnp.float32)
    if pieces:
        drawn = drawn * shard_levels(rng, shape, pieces, -0.22, 0.18)
    return jnp.clip(drawn, -reach, reach).astype(held_as)


def setup_inputs(seed: int = 0) -> dict:
    key_of = jax.random.split(jax.random.key(seed), 9)
    return {
        "fine_residual": scatter_about(key_of[0], (INST, VARS, FINE), 1.0, 6.0, ((0, 4), (2, 8)), jnp.float32),
        "fine_map": touch_ends(jax.random.randint(key_of[1], (FINE,), 0, BLK // AGG), jax.random.fold_in(key_of[1], 1), 0, (BLK // AGG) - 1).astype(jnp.int32),
        "routes": draw_routes(jax.random.fold_in(key_of[8], 71), 0),
        "receive_lists": touch_ends(jax.random.randint(key_of[3], (N_CELL, 2 * RAD * HS), 0, CC), jax.random.fold_in(key_of[3], 1), 0, CC - 1).astype(jnp.int32),
        "neighbours": draw_neighbours(jax.random.fold_in(key_of[8], 71), 0),
        "face_weights": jnp.clip(jnp.exp(math.log(3.0) - 2.3025851 * jax.random.uniform(key_of[5], (NB, COARSE), jnp.float32) ** shard_levels(key_of[5], (NB, COARSE), ((1, 8),), -0.2, 0.2)), 0.3, 3.0),
        "spectral_coef": jnp.clip(jnp.exp(math.log(1.0) - 1.609438 * jax.random.uniform(key_of[6], (COARSE,), jnp.float32) ** shard_levels(key_of[6], (COARSE,), ((0, 8),), -0.2, 0.2)), 0.2, 1.0),
        "diag_extra": jnp.clip(jnp.exp(math.log(2.0) - 1.3862944 * jax.random.uniform(key_of[7], (VARS, COARSE), jnp.float32) ** shard_levels(key_of[7], (VARS, COARSE), ((1, 8),), -0.2, 0.2)), 0.5, 2.0),
    }


exact_precision = lax.Precision.HIGHEST


def spectral_matrix():
    row_ids = jnp.arange(INST)[:, None]
    col_ids = jnp.arange(INST)[None, :]
    distance = row_ids - col_ids
    usable = (row_ids < HB_INST) & (col_ids < HB_INST) & (distance != 0)
    parity = 1.0 - 2.0 * jnp.mod(distance, 2).astype(jnp.float32)
    denominator = jnp.sin(jnp.pi * jnp.where(usable, distance, 1).astype(jnp.float32) / HB_INST)
    return jnp.where(usable, 0.5 * parity / denominator, 0.0).astype(jnp.float32)


def reference(fine_residual, fine_map, routes, receive_lists, neighbours, face_weights, spectral_coef, diag_extra):
    source = jnp.arange(N_CELL, dtype=jnp.int32)[:, None]
    relative = jnp.mod(routes - source, N_CELL)
    category = jnp.where(relative == 1, 0, jnp.where(relative == 0, 1, 2)).astype(jnp.int32)
    block_order = jnp.argsort(category, axis=1, stable=True).astype(jnp.int32)
    position = jnp.argsort(block_order, axis=1, stable=True).astype(jnp.int32)
    block_base = routes * CC + position * CBLK
    coarse_of_fine = (block_base[:, :, None] + fine_map.reshape(N_CELL, FB, BLK)).reshape(-1).astype(jnp.int32)
    flat_fine = fine_residual.reshape(INST * VARS, FINE).T
    coarse_residual = jax.ops.segment_sum(flat_fine, coarse_of_fine, num_segments=COARSE).T.reshape(INST, VARS, COARSE)
    inst_ids = jnp.arange(INST)
    coarse_residual = jnp.where((inst_ids < HB_INST)[:, None, None], coarse_residual, jnp.float32(0.0))
    owners = (jnp.arange(COARSE, dtype=jnp.int32) // CC)[None, :]
    is_local = neighbours < CC
    halo_slot = jnp.maximum(neighbours - CC, 0)
    peer_slot = halo_slot // HS
    offset = jnp.where(peer_slot < RAD, peer_slot - RAD, peer_slot - RAD + 1)
    sender = jnp.mod(owners + offset, N_CELL)
    remote_index = receive_lists[jnp.broadcast_to(owners, neighbours.shape), halo_slot]
    neighbour_ids = jnp.where(is_local, owners * CC + neighbours, sender * CC + remote_index).astype(jnp.int32)
    diagonal = jnp.sum(face_weights, axis=0)[None, :] + 3.0 * spectral_coef[None, :] + diag_extra
    spectral = spectral_matrix()
    correction = coarse_residual / diagonal[None]
    for sweep in range(ITERS):
        neighbour_sum = jnp.zeros_like(correction)
        for slot_index in range(NB):
            neighbour_sum = neighbour_sum + face_weights[slot_index][None, None, :] * jnp.take(correction, neighbour_ids[slot_index], axis=2)
        coupling = jnp.einsum("nm,mvc->nvc", spectral, correction, precision=exact_precision)
        correction = (coarse_residual + neighbour_sum - spectral_coef[None, None, :] * coupling) / diagonal[None]
    fine_correction = jnp.take(correction, coarse_of_fine, axis=2)
    return fine_correction, correction
```

```python
import functools
import math

import jax
import jax.numpy as jnp
from jax import lax
from jax.experimental import pallas as pl
from jax.experimental.pallas import tpu as pltpu
from jax.sharding import PartitionSpec as P

INST = 8
HB_INST = 7
AGG = 8
BLK = 128
RAD = 3
ITERS = 6
LANES = 128
MESH = pl.DeviceIdType.MESH
CBLK = BLK // AGG
PER_TILE = LANES // CBLK

OFFSETS = [slot - RAD if slot < RAD else slot - RAD + 1 for slot in range(2 * RAD)]
NN = (((1,), (0,)), ((), ()))
NT = (((1,), (1,)), ((), ()))


def dot(a, b, dims=NN):
    return lax.dot_general(a, b, dims, preferred_element_type=jnp.float32)


def split(x):
    hi = x.astype(jnp.bfloat16)
    return hi, (x - hi.astype(jnp.float32)).astype(jnp.bfloat16)


def stack(x):
    return jnp.concatenate(split(x), axis=0)


def fold(y):
    half = y.shape[0] // 2
    return y[:half] + y[half:]


def iota(shape, dim):
    return lax.broadcasted_iota(jnp.int32, shape, dim)


def as_bf16(mask):
    return jnp.where(mask, 1.0, 0.0).astype(jnp.bfloat16)


def spectral_block(rows):
    shape = (rows, 3 * rows)
    row, col = iota(shape, 0), iota(shape, 1)
    part, m = col // rows, col % rows
    same = (row // INST == m // INST) & (row % INST < HB_INST) & (m % INST < HB_INST)
    dist = row % INST - m % INST
    full = jnp.zeros(shape, jnp.float32)
    for d in range(1 - HB_INST, HB_INST):
        if d:
            value = 0.5 * (-1.0) ** d / math.sin(math.pi * d / HB_INST)
            full = jnp.where(same & (dist == d), jnp.float32(value), full)
    hi, lo = split(full)
    return jnp.where(part < 2, hi.astype(jnp.float32), lo.astype(jnp.float32)).astype(jnp.bfloat16)


def kernel(
    n_cell, n_inst, vpd,
    fine_ref, map_ref, routes_ref, lists_ref, nb_ref, w_ref, sc_ref, de_ref,
    fine_out, coarse_out,
    e_ref, q_ref, ahi, alo, s_ref,
    sbuf, rbuf, rlo, rhi, lbuf, obuf, hbuf, fbuf, gbuf, glo, ghi,
    a_send, a_recv, l_send, l_recv, h_send, h_recv, f_send, f_recv,
):
    inst_dev, n_var, _ = fine_ref.shape
    coarse = nb_ref.shape[1]
    blocks = routes_ref.shape[1]
    hw = lists_ref.shape[1] // (2 * RAD)
    per = LANES // hw
    n_halo = s_ref.shape[1]
    halo_tiles = n_halo // LANES
    handed = blocks // 16 * CBLK
    groups = blocks // PER_TILE
    span = PER_TILE * BLK
    pad_var = vpd * n_inst
    rows = vpd * INST
    cell = lax.axis_index("cell")
    me = lax.axis_index("inst")

    def at(dc, inst):
        return {"cell": lax.rem(cell + (dc + n_cell), n_cell), "inst": inst}

    def other(k):
        return lax.rem(me + k, n_inst)

    barrier = pltpu.get_barrier_semaphore()
    greeted = [(d, 0) for d in OFFSETS]
    greeted += [(d, k) for d in (-1, 0, 1) for k in range(n_inst) if k]
    for d, k in greeted:
        pl.semaphore_signal(barrier, inc=1, device_id=at(d, other(k)), device_id_type=MESH)

    lane = iota((1, span), 1)
    sub = iota((LANES, span), 0)
    parts = []
    for g in range(groups):
        want = map_ref[:, g * span:(g + 1) * span] + (lane // BLK) * CBLK
        e_ref[g] = as_bf16(sub == want)
        x = fine_ref[:, :, g * span:(g + 1) * span]
        pieces = []
        for i in range(inst_dev):
            pieces.append(x[i])
            if pad_var > n_var:
                pieces.append(jnp.zeros((pad_var - n_var, span), jnp.float32))
        x = jnp.concatenate(pieces, axis=0)
        parts.append(fold(dot(stack(x), e_ref[g], NT)))
    y = jnp.concatenate(parts, axis=1)

    rel = lax.rem(routes_ref[...] - cell + n_cell, n_cell)
    kinds = [(rel == 1), (rel == 0), (rel != 1) & (rel != 0)]
    ind = [jnp.where(k, 1.0, 0.0) for k in kinds]
    tri = as_bf16(iota((blocks, blocks), 0) < iota((blocks, blocks), 1))
    pos = jnp.zeros((1, blocks), jnp.float32)
    base = jnp.zeros((1, 1), jnp.float32)
    for k in ind:
        before = dot(jnp.broadcast_to(k, (16, blocks)).astype(jnp.bfloat16), tri)[:1]
        pos = pos + k * (before + base)
        base = base + jnp.sum(k, axis=1, keepdims=True)
    rep = as_bf16(iota((blocks, coarse), 0) == iota((blocks, coarse), 1) // CBLK)
    pos = dot(jnp.broadcast_to(pos, (16, blocks)).astype(jnp.bfloat16), rep)[:1]
    target = pos.astype(jnp.int32) * CBLK + iota((1, coarse), 1) % CBLK
    q_ref[...] = as_bf16(iota((coarse, coarse), 0) == target)

    row = iota((inst_dev * pad_var, 1), 0)
    live = me * inst_dev + row // pad_var < HB_INST
    y = jnp.where(live, fold(dot(stack(y), q_ref[...], NT)), 0.0)
    for j in range(n_inst):
        picked = []
        for v in range(vpd):
            for i in range(inst_dev):
                r = i * pad_var + j * vpd + v
                picked.append(y[r:r + 1])
        sbuf[j] = jnp.concatenate(picked, axis=0)

    pl.semaphore_wait(barrier, len(greeted))

    def remote(src, dst, send, recv, dc, inst):
        copy = pltpu.make_async_remote_copy(
            src_ref=src, dst_ref=dst, send_sem=send, recv_sem=recv,
            device_id=at(dc, inst), device_id_type=MESH)
        copy.start()
        return copy

    def swap(src, mid, low, high, send, recv, dc):
        copies = []
        for k in range(n_inst):
            j = other(k)
            if k:
                copies.append(remote(src.at[j], mid.at[me], send.at[0, k], recv.at[0, k], 0, j))
            copies.append(remote(
                src.at[j, :, pl.ds(0, LANES)], low.at[me], send.at[1, k], recv.at[1, k], dc, j))
            copies.append(remote(
                src.at[j, :, pl.ds(coarse - LANES, LANES)], high.at[me],
                send.at[2, k], recv.at[2, k], -dc, j))
        mid[me] = src[me]
        return copies

    list_copies = [
        remote(lists_ref, lbuf.at[t], l_send.at[t], l_recv.at[t], OFFSETS[t], me)
        for t in range(2 * RAD)]
    swaps = swap(sbuf, rbuf, rlo, rhi, a_send, a_recv, 1)

    chunk = 64

    def build(k, carry):
        at_row = pl.multiple_of(k * chunk, chunk)
        ids = iota((chunk, coarse), 0) + k * chunk
        total = jnp.zeros((chunk, coarse), jnp.float32)
        for s in range(nb_ref.shape[0]):
            total = total + jnp.where(nb_ref[s:s + 1] == ids, w_ref[s:s + 1], 0.0)
        hi, lo = split(total)
        ahi[pl.ds(at_row, chunk)] = hi
        alo[pl.ds(at_row, chunk)] = lo
        return carry

    lax.fori_loop(0, (coarse + n_halo) // chunk, build, 0)

    sc = sc_ref[...]
    wsum = jnp.sum(w_ref[...], axis=0, keepdims=True) + 3.0 * sc
    diags = []
    for v in range(vpd):
        extra = jnp.zeros_like(sc)
        for var in range(n_var):
            extra = jnp.where(me * vpd + v == var, de_ref[var:var + 1], extra)
        diags.append(jnp.broadcast_to(wsum + extra, (INST, coarse)))
    rinv = 1.0 / jnp.concatenate(diags, axis=0)
    scr = sc * rinv
    spec = spectral_block(rows)

    lane = iota((1, LANES), 1)

    def pick(tile, get):
        value = get(tile * per)
        for t in range(tile * per + 1, min((tile + 1) * per, 2 * RAD)):
            value = jnp.where(lane // hw == t % per, get(t), value)
        return value

    for copy in list_copies:
        copy.wait()
    sub = iota((coarse, LANES), 0)
    for tile in range(halo_tiles):
        def listed(t):
            value = lbuf[t]
            width = value.shape[1]
            start = tile * LANES
            if start + LANES <= width:
                return value[:, start:start + LANES]
            return jnp.concatenate(
                [value[:, start:], jnp.zeros((1, start + LANES - width), jnp.int32)], axis=1)
        s_ref[:, tile * LANES:(tile + 1) * LANES] = as_bf16(sub == pick(tile, listed))

    for copy in swaps:
        copy.wait()
    wide = iota((1, coarse), 1)

    def edges(whole, low, high):
        fill = jnp.zeros((whole.shape[0], coarse - LANES), jnp.float32)
        low = jnp.concatenate([low, fill], axis=1)
        high = jnp.concatenate([fill, high], axis=1)
        return jnp.where(wide < handed, low, jnp.where(wide >= coarse - handed, high, whole))

    def ordered(buf):
        return jnp.concatenate(
            [buf[i, v * inst_dev:(v + 1) * inst_dev] for v in range(vpd) for i in range(n_inst)],
            axis=0)

    first = edges(ordered(rbuf), ordered(rlo), ordered(rhi)) * rinv

    def sweep(s, x):
        hi, lo = split(x)
        both = jnp.concatenate([hi, lo], axis=0)
        out = fold(dot(both, s_ref[...]))
        for tile in range(halo_tiles):
            obuf[s, tile] = out[:, tile * LANES:(tile + 1) * LANES]
        copies = [
            remote(obuf.at[s, t // per], hbuf.at[s, t], h_send.at[s, t], h_recv.at[s, t],
                   -OFFSETS[t], me)
            for t in range(2 * RAD)]
        total = fold(dot(both, ahi[:coarse])) + dot(hi, alo[:coarse])
        coupled = dot(spec, jnp.concatenate([hi, lo, hi], axis=0))
        partial = first + total * rinv - coupled * scr
        for copy in copies:
            copy.wait()
        halo = jnp.concatenate(
            [pick(tile, lambda t: hbuf[s, t]) for tile in range(halo_tiles)], axis=1)
        hi, lo = split(halo)
        both = jnp.concatenate([hi, lo], axis=0)
        return partial + rinv * (fold(dot(both, ahi[coarse:])) + dot(hi, alo[coarse:]))

    x = lax.fori_loop(0, ITERS, sweep, first)

    for i in range(n_inst):
        fbuf[i] = jnp.concatenate(
            [x[v * INST + i * inst_dev:v * INST + (i + 1) * inst_dev] for v in range(vpd)], axis=0)
    swaps = swap(fbuf, gbuf, glo, ghi, f_send, f_recv, -1)
    for copy in swaps:
        copy.wait()

    def by_var(buf):
        return jnp.concatenate(
            [buf[j, v * inst_dev + i:v * inst_dev + i + 1]
             for i in range(inst_dev) for j in range(n_inst) for v in range(vpd)], axis=0)

    whole = by_var(gbuf)
    for i in range(inst_dev):
        coarse_out[i] = whole[i * pad_var:i * pad_var + n_var]
    back = dot(stack(edges(whole, by_var(glo), by_var(ghi))), q_ref[...]).astype(jnp.bfloat16)
    for g in range(groups):
        fine = fold(dot(back[:, g * LANES:(g + 1) * LANES], e_ref[g]))
        for i in range(inst_dev):
            fine_out[i, :, g * span:(g + 1) * span] = fine[i * pad_var:i * pad_var + n_var]


def body(n_cell, n_inst, fine_residual, fine_map, routes, receive_lists, neighbours,
         face_weights, spectral_coef, diag_extra):
    inst_dev, n_var, fine_dev = fine_residual.shape
    coarse = neighbours.shape[1]
    blocks = routes.shape[1]
    halo = receive_lists.shape[1]
    n_halo = -(-halo // LANES) * LANES
    vpd = -(-n_var // n_inst)
    rows = vpd * INST
    part = vpd * inst_dev
    f32, bf16 = jnp.float32, jnp.bfloat16
    vmem = pl.BlockSpec(memory_space=pltpu.VMEM)
    dma = pltpu.SemaphoreType.DMA
    return pl.pallas_call(
        functools.partial(kernel, n_cell, n_inst, vpd),
        out_shape=(
            jax.ShapeDtypeStruct(fine_residual.shape, f32),
            jax.ShapeDtypeStruct((inst_dev, n_var, coarse), f32),
        ),
        in_specs=[vmem] * 8,
        out_specs=(vmem, vmem),
        scratch_shapes=[
            pltpu.VMEM((blocks // PER_TILE, LANES, PER_TILE * BLK), bf16),
            pltpu.VMEM((coarse, coarse), bf16),
            pltpu.VMEM((coarse + n_halo, coarse), bf16),
            pltpu.VMEM((coarse + n_halo, coarse), bf16),
            pltpu.VMEM((coarse, n_halo), bf16),
            pltpu.VMEM((n_inst, part, coarse), f32),
            pltpu.VMEM((n_inst, part, coarse), f32),
            pltpu.VMEM((n_inst, part, LANES), f32),
            pltpu.VMEM((n_inst, part, LANES), f32),
            pltpu.VMEM((2 * RAD, 1, halo), jnp.int32),
            pltpu.VMEM((ITERS, n_halo // LANES, rows, LANES), f32),
            pltpu.VMEM((ITERS, 2 * RAD, rows, LANES), f32),
            pltpu.VMEM((n_inst, part, coarse), f32),
            pltpu.VMEM((n_inst, part, coarse), f32),
            pltpu.VMEM((n_inst, part, LANES), f32),
            pltpu.VMEM((n_inst, part, LANES), f32),
            dma((3, n_inst)), dma((3, n_inst)),
            dma((2 * RAD,)), dma((2 * RAD,)),
            dma((ITERS, 2 * RAD)), dma((ITERS, 2 * RAD)),
            dma((3, n_inst)), dma((3, n_inst)),
        ],
        compiler_params=pltpu.CompilerParams(
            collective_id=0, has_side_effects=True, vmem_limit_bytes=48 * 1024 * 1024),
        name="multigrid",
    )(fine_residual, fine_map.reshape(1, -1), routes, receive_lists, neighbours,
      face_weights, spectral_coef.reshape(1, -1), diag_extra)


def solution(mesh):
    in_specs = (
        P("inst", None, "cell"),
        P("cell"),
        P("cell", None),
        P("cell", None),
        P(None, "cell"),
        P(None, "cell"),
        P("cell"),
        P(None, "cell"),
    )
    out_specs = (P("inst", None, "cell"), P("inst", None, "cell"))
    run = functools.partial(body, mesh.shape["cell"], mesh.shape["inst"])
    return jax.shard_map(run, mesh=mesh, in_specs=in_specs, out_specs=out_specs, check_vma=False)
```

```python
import functools
import math

import jax
import jax.numpy as jnp
from jax import lax
from jax.experimental import pallas as pl
from jax.experimental.pallas import tpu as pltpu
from jax.sharding import PartitionSpec as P

INST = 8
HB_INST = 7
AGG = 8
BLK = 128
RAD = 3
ITERS = 6
LANES = 128
MESH = pl.DeviceIdType.MESH
CBLK = BLK // AGG
PER_TILE = LANES // CBLK

OFFSETS = [slot - RAD if slot < RAD else slot - RAD + 1 for slot in range(2 * RAD)]
NN = (((1,), (0,)), ((), ()))
NT = (((1,), (1,)), ((), ()))


def dot(a, b, dims=NN):
    return lax.dot_general(a, b, dims, preferred_element_type=jnp.float32)


def split(x):
    hi = x.astype(jnp.bfloat16)
    return hi, (x - hi.astype(jnp.float32)).astype(jnp.bfloat16)


def stack(x):
    return jnp.concatenate(split(x), axis=0)


def fold(y):
    half = y.shape[0] // 2
    return y[:half] + y[half:]


def iota(shape, dim):
    return lax.broadcasted_iota(jnp.int32, shape, dim)


def as_bf16(mask):
    return jnp.where(mask, 1.0, 0.0).astype(jnp.bfloat16)


def spectral_block(rows):
    shape = (rows, 3 * rows)
    row, col = iota(shape, 0), iota(shape, 1)
    part, m = col // rows, col % rows
    same = (row // INST == m // INST) & (row % INST < HB_INST) & (m % INST < HB_INST)
    dist = row % INST - m % INST
    full = jnp.zeros(shape, jnp.float32)
    for d in range(1 - HB_INST, HB_INST):
        if d:
            value = 0.5 * (-1.0) ** d / math.sin(math.pi * d / HB_INST)
            full = jnp.where(same & (dist == d), jnp.float32(value), full)
    hi, lo = split(full)
    return jnp.where(part < 2, hi.astype(jnp.float32), lo.astype(jnp.float32)).astype(jnp.bfloat16)


class Layout:
    def __init__(self, n_cell, n_inst):
        self.n_cell, self.n_inst = n_cell, n_inst
        self.half = n_cell // 2
        even = n_cell % 2 == 0 and n_inst % 2 == 0
        self.folded = even and RAD < self.half <= 2 * RAD

    def worker(self, part, group):
        if not self.folded:
            return part, group
        wide = self.n_inst // 2
        up, right = part >= self.half, group >= wide
        cell = jnp.where(up, part - self.half, part) + jnp.where(right, self.half, 0)
        return cell, 2 * jnp.where(right, group - wide, group) + jnp.where(up, 1, 0)

    def role(self, cell, inst):
        if not self.folded:
            return cell, inst
        up = cell >= self.half
        core = lax.rem(inst, 2)
        part = core * self.half + jnp.where(up, cell - self.half, cell)
        return part, jnp.where(up, self.n_inst // 2, 0) + lax.div(inst, 2)

    def served(self, inst):
        if not self.folded:
            return inst
        return lax.div(inst, 2) + lax.rem(inst, 2) * (self.n_inst // 2)


def wrap(value, count):
    value = jnp.where(value >= count, value - count, value)
    return jnp.where(value < 0, value + count, value)


def kernel(
    n_cell, n_inst, vpd,
    fine_ref, map_ref, routes_ref, lists_ref, nb_in, w_in, sc_in, de_in,
    fine_out, coarse_out,
    nb_ref, w_ref, sc_ref, de_ref, e_ref, q_ref, ahi, alo, s_ref,
    sbuf, rbuf, rlo, rhi, lbuf, obuf, hbuf, fbuf, gbuf, glo, ghi,
    w_send, w_recv, a_send, a_recv, l_send, l_recv, h_send, h_recv, f_send, f_recv,
):
    inst_dev, n_var, _ = fine_ref.shape
    coarse = nb_in.shape[1]
    blocks = routes_ref.shape[1]
    hw = lists_ref.shape[1] // (2 * RAD)
    per = LANES // hw
    n_halo = s_ref.shape[1]
    halo_tiles = n_halo // LANES
    handed = blocks // 16 * CBLK
    groups = blocks // PER_TILE
    span = PER_TILE * BLK
    pad_var = vpd * n_inst
    rows = vpd * INST
    cell = lax.axis_index("cell")
    me = lax.axis_index("inst")

    lay = Layout(n_cell, n_inst)
    part, group = lay.role(cell, me)
    devices = n_cell * n_inst
    barrier = pltpu.get_barrier_semaphore()

    def greet(k, carry):
        for i in range(1 if isinstance(k, int) else 0, n_inst):
            pl.semaphore_signal(
                barrier, inc=1, device_id_type=MESH,
                device_id={"cell": wrap(cell + k, n_cell), "inst": wrap(me + i, n_inst)})
        return carry

    greet(0, 0)
    lax.fori_loop(1, n_cell, greet, 0)

    lane = iota((1, span), 1)
    sub = iota((LANES, span), 0)
    parts = []
    for g in range(groups):
        want = map_ref[:, g * span:(g + 1) * span] + (lane // BLK) * CBLK
        e_ref[g] = as_bf16(sub == want)
        x = fine_ref[:, :, g * span:(g + 1) * span]
        pieces = [x[i, v:v + 1] for v in range(n_var) for i in range(inst_dev)]
        if pad_var > n_var:
            pieces.append(jnp.zeros(((pad_var - n_var) * inst_dev, span), jnp.float32))
        x = jnp.concatenate(pieces, axis=0)
        parts.append(fold(dot(stack(x), e_ref[g], NT)))
    y = jnp.concatenate(parts, axis=1)

    def remote(src, dst, send, recv, where):
        return pltpu.make_async_remote_copy(
            src_ref=src, dst_ref=dst, send_sem=send, recv_sem=recv,
            device_id={"cell": where[0], "inst": where[1]}, device_id_type=MESH)

    def away(where, then):
        pl.when((where[0] != cell) | (where[1] != me))(then)

    def home(where, then):
        pl.when((where[0] == cell) & (where[1] == me))(then)

    def near(p, d):
        return wrap(p + d, n_cell)

    def swap(src, mid, low, high, send, recv, slot, target, dc, source):
        first, last = pl.ds(0, LANES), pl.ds(coarse - LANES, LANES)
        for k in range(n_inst):
            where = target(0, k)
            copy = remote(src.at[k], mid.at[slot], send.at[0, k], recv.at[0, slot], where)
            away(where, copy.start)

            def keep():
                mid[slot] = src[k]

            home(where, keep)
            remote(src.at[k, :, first], low.at[slot], send.at[1, k], recv.at[1, slot],
                   target(dc, k)).start()
            remote(src.at[k, :, last], high.at[slot], send.at[2, k], recv.at[2, slot],
                   target(-dc, k)).start()

        def finish():
            for k in range(n_inst):
                arrival = remote(src.at[k], mid.at[k], send.at[0, k], recv.at[0, k], source(k))
                away(source(k), arrival.wait_recv)
                away(target(0, k), arrival.wait_send)
                remote(src.at[k, :, first], low.at[k], send.at[1, k], recv.at[1, k],
                       target(dc, k)).wait()
                remote(src.at[k, :, last], high.at[k], send.at[2, k], recv.at[2, k],
                       target(-dc, k)).wait()

        return finish

    rel = lax.rem(routes_ref[...] - cell + n_cell, n_cell)
    kinds = [(rel == 1), (rel == 0), (rel != 1) & (rel != 0)]
    ind = [jnp.where(k, 1.0, 0.0) for k in kinds]
    tri = as_bf16(iota((blocks, blocks), 0) < iota((blocks, blocks), 1))
    pos = jnp.zeros((1, blocks), jnp.float32)
    base = jnp.zeros((1, 1), jnp.float32)
    for k in ind:
        before = dot(jnp.broadcast_to(k, (16, blocks)).astype(jnp.bfloat16), tri)[:1]
        pos = pos + k * (before + base)
        base = base + jnp.sum(k, axis=1, keepdims=True)
    rep = as_bf16(iota((blocks, coarse), 0) == iota((blocks, coarse), 1) // CBLK)
    pos = dot(jnp.broadcast_to(pos, (16, blocks)).astype(jnp.bfloat16), rep)[:1]
    target = pos.astype(jnp.int32) * CBLK + iota((1, coarse), 1) % CBLK
    q_ref[...] = as_bf16(iota((coarse, coarse), 0) == target)

    pl.semaphore_wait(barrier, devices - 1)

    mine = lay.served(me)
    weights = [(nb_in, nb_ref), (w_in, w_ref), (sc_in, sc_ref), (de_in, de_ref)]
    if lay.folded:
        goal = lay.worker(cell, mine)
        weight_copies = [
            remote(src, dst, w_send.at[n], w_recv.at[n], goal)
            for n, (src, dst) in enumerate(weights)]

        def send_weights():
            for copy in weight_copies:
                copy.start()

        def keep_weights():
            for src, dst in weights:
                dst[...] = src[...]

        away(goal, send_weights)
        home(goal, keep_weights)
    else:
        for src, dst in weights:
            dst[...] = src[...]

    list_copies = [
        remote(lists_ref, lbuf.at[t], l_send.at[t], l_recv.at[t],
               lay.worker(near(cell, OFFSETS[t]), mine))
        for t in range(2 * RAD)]
    for copy in list_copies:
        copy.start()

    row = iota((inst_dev * pad_var, 1), 0)
    live = me * inst_dev + row % inst_dev < HB_INST
    y = jnp.where(live, fold(dot(stack(y), q_ref[...], NT)), 0.0)
    width = vpd * inst_dev
    for j in range(n_inst):
        sbuf[j] = y[j * width:(j + 1) * width]
    arrive = swap(sbuf, rbuf, rlo, rhi, a_send, a_recv, me,
                  lambda d, k: lay.worker(near(cell, d), k), 1, lambda k: (part, k))

    if lay.folded:
        def take_weights():
            for copy in weight_copies:
                copy.wait_recv()

        def sent_weights():
            for copy in weight_copies:
                copy.wait_send()

        origin = (part, lax.div(me, 2) * 2 + jnp.where(cell >= lay.half, 1, 0))
        away(origin, take_weights)
        away(goal, sent_weights)

    chunk = 64

    def build(k, carry):
        at_row = pl.multiple_of(k * chunk, chunk)
        ids = iota((chunk, coarse), 0) + k * chunk
        total = jnp.zeros((chunk, coarse), jnp.float32)
        for s in range(nb_ref.shape[0]):
            total = total + jnp.where(nb_ref[s:s + 1] == ids, w_ref[s:s + 1], 0.0)
        hi, lo = split(total)
        ahi[pl.ds(at_row, chunk)] = hi
        alo[pl.ds(at_row, chunk)] = lo
        return carry

    lax.fori_loop(0, (coarse + n_halo) // chunk, build, 0)

    sc = sc_ref[...]
    wsum = jnp.sum(w_ref[...], axis=0, keepdims=True) + 3.0 * sc
    diags = []
    for v in range(vpd):
        extra = jnp.zeros_like(sc)
        for var in range(n_var):
            extra = jnp.where(group * vpd + v == var, de_ref[var:var + 1], extra)
        diags.append(jnp.broadcast_to(wsum + extra, (INST, coarse)))
    rinv = 1.0 / jnp.concatenate(diags, axis=0)
    scr = sc * rinv
    spec = spectral_block(rows)

    lane = iota((1, LANES), 1)

    def pick(tile, get):
        value = get(tile * per)
        for t in range(tile * per + 1, min((tile + 1) * per, 2 * RAD)):
            value = jnp.where(lane // hw == t % per, get(t), value)
        return value

    for copy in list_copies:
        copy.wait()
    sub = iota((coarse, LANES), 0)
    for tile in range(halo_tiles):
        def listed(t):
            value = lbuf[t]
            width = value.shape[1]
            start = tile * LANES
            if start + LANES <= width:
                return value[:, start:start + LANES]
            return jnp.concatenate(
                [value[:, start:], jnp.zeros((1, start + LANES - width), jnp.int32)], axis=1)
        s_ref[:, tile * LANES:(tile + 1) * LANES] = as_bf16(sub == pick(tile, listed))

    arrive()
    wide = iota((1, coarse), 1)

    def edges(whole, low, high):
        fill = jnp.zeros((whole.shape[0], coarse - LANES), jnp.float32)
        low = jnp.concatenate([low, fill], axis=1)
        high = jnp.concatenate([fill, high], axis=1)
        return jnp.where(wide < handed, low, jnp.where(wide >= coarse - handed, high, whole))

    def ordered(buf):
        return jnp.concatenate(
            [buf[i, v * inst_dev:(v + 1) * inst_dev] for v in range(vpd) for i in range(n_inst)],
            axis=0)

    first = edges(ordered(rbuf), ordered(rlo), ordered(rhi)) * rinv

    peers = [lay.worker(near(part, -d), group) for d in OFFSETS]

    def sweep(s, x):
        hi, lo = split(x)
        both = jnp.concatenate([hi, lo], axis=0)
        out = fold(dot(both, s_ref[...]))
        for tile in range(halo_tiles):
            obuf[s, tile] = out[:, tile * LANES:(tile + 1) * LANES]
        copies = [
            remote(obuf.at[s, t // per], hbuf.at[s, t], h_send.at[s, t], h_recv.at[s, t],
                   peers[t])
            for t in range(2 * RAD)]
        for copy in copies:
            copy.start()
        total = fold(dot(both, ahi[:coarse])) + dot(hi, alo[:coarse])
        coupled = dot(spec, jnp.concatenate([hi, lo, hi], axis=0))
        partial = first + total * rinv - coupled * scr
        for copy in copies:
            copy.wait()
        halo = jnp.concatenate(
            [pick(tile, lambda t: hbuf[s, t]) for tile in range(halo_tiles)], axis=1)
        hi, lo = split(halo)
        both = jnp.concatenate([hi, lo], axis=0)
        return partial + rinv * (fold(dot(both, ahi[coarse:])) + dot(hi, alo[coarse:]))

    x = lax.fori_loop(0, ITERS, sweep, first)

    for i in range(n_inst):
        fbuf[i] = jnp.concatenate(
            [x[v * INST + i * inst_dev:v * INST + (i + 1) * inst_dev] for v in range(vpd)], axis=0)
    arrive = swap(fbuf, gbuf, glo, ghi, f_send, f_recv, group,
                  lambda d, k: (near(part, d), k), -1, lambda k: lay.worker(cell, k))
    arrive()

    def by_var(buf):
        return jnp.concatenate([buf[j] for j in range(n_inst)], axis=0)

    whole = by_var(gbuf)
    for v in range(n_var):
        for i in range(inst_dev):
            coarse_out[i, v:v + 1] = whole[v * inst_dev + i:v * inst_dev + i + 1]
    back = dot(stack(edges(whole, by_var(glo), by_var(ghi))), q_ref[...]).astype(jnp.bfloat16)
    for g in range(groups):
        fine = fold(dot(back[:, g * LANES:(g + 1) * LANES], e_ref[g]))
        for v in range(n_var):
            for i in range(inst_dev):
                r = v * inst_dev + i
                fine_out[i, v:v + 1, g * span:(g + 1) * span] = fine[r:r + 1]


def body(n_cell, n_inst, fine_residual, fine_map, routes, receive_lists, neighbours,
         face_weights, spectral_coef, diag_extra):
    inst_dev, n_var, fine_dev = fine_residual.shape
    coarse = neighbours.shape[1]
    blocks = routes.shape[1]
    halo = receive_lists.shape[1]
    n_halo = -(-halo // LANES) * LANES
    vpd = -(-n_var // n_inst)
    rows = vpd * INST
    part = vpd * inst_dev
    f32, bf16 = jnp.float32, jnp.bfloat16
    vmem = pl.BlockSpec(memory_space=pltpu.VMEM)
    dma = pltpu.SemaphoreType.DMA
    fine_correction, correction = pl.pallas_call(
        functools.partial(kernel, n_cell, n_inst, vpd),
        out_shape=(
            jax.ShapeDtypeStruct(fine_residual.shape, f32),
            jax.ShapeDtypeStruct((inst_dev, n_var, coarse), f32),
        ),
        in_specs=[vmem] * 8,
        out_specs=(vmem, vmem),
        scratch_shapes=[
            pltpu.VMEM(neighbours.shape, jnp.int32),
            pltpu.VMEM(face_weights.shape, f32),
            pltpu.VMEM((1, coarse), f32),
            pltpu.VMEM(diag_extra.shape, f32),
            pltpu.VMEM((blocks // PER_TILE, LANES, PER_TILE * BLK), bf16),
            pltpu.VMEM((coarse, coarse), bf16),
            pltpu.VMEM((coarse + n_halo, coarse), bf16),
            pltpu.VMEM((coarse + n_halo, coarse), bf16),
            pltpu.VMEM((coarse, n_halo), bf16),
            pltpu.VMEM((n_inst, part, coarse), f32),
            pltpu.VMEM((n_inst, part, coarse), f32),
            pltpu.VMEM((n_inst, part, LANES), f32),
            pltpu.VMEM((n_inst, part, LANES), f32),
            pltpu.VMEM((2 * RAD, 1, halo), jnp.int32),
            pltpu.VMEM((ITERS, n_halo // LANES, rows, LANES), f32),
            pltpu.VMEM((ITERS, 2 * RAD, rows, LANES), f32),
            pltpu.VMEM((n_inst, part, coarse), f32),
            pltpu.VMEM((n_inst, part, coarse), f32),
            pltpu.VMEM((n_inst, part, LANES), f32),
            pltpu.VMEM((n_inst, part, LANES), f32),
            dma((4,)), dma((4,)),
            dma((3, n_inst)), dma((3, n_inst)),
            dma((2 * RAD,)), dma((2 * RAD,)),
            dma((ITERS, 2 * RAD)), dma((ITERS, 2 * RAD)),
            dma((3, n_inst)), dma((3, n_inst)),
        ],
        compiler_params=pltpu.CompilerParams(
            collective_id=0, has_side_effects=True, vmem_limit_bytes=48 * 1024 * 1024),
        name="multigrid",
    )(fine_residual, fine_map.reshape(1, -1), routes, receive_lists, neighbours,
      face_weights, spectral_coef.reshape(1, -1), diag_extra)
    return fine_correction, correction


def solution(mesh):
    in_specs = (
        P("inst", None, "cell"),
        P("cell"),
        P("cell", None),
        P("cell", None),
        P(None, "cell"),
        P(None, "cell"),
        P("cell"),
        P(None, "cell"),
    )
    out_specs = (P("inst", None, "cell"), P("inst", None, "cell"))
    run = functools.partial(body, mesh.shape["cell"], mesh.shape["inst"])
    return jax.shard_map(run, mesh=mesh, in_specs=in_specs, out_specs=out_specs, check_vma=False)
```
